256 devices in a mesh: table: 4 (over z_lo), row: 64 (over z_hi, y, x, core).
Axes of the slice: x: 4, y: 4, z: 8 (z_hi: 2, z_lo: 4; z = z_hi * 4 + z_lo), core: 2. Of those that a mesh axis runs over, the one named last changes fastest.
Arguments:
- tables: bfloat16 [4, 524288, 128], P('table', 'row'), may hold values from -3 to 3
- indices: int32 [4, 100, 512], P('table'), may hold values from 0 to 524287
- weights: bfloat16 [4, 100, 512], P('table'), may hold values from 0.19921875 to 1
- lengths: int32 [4, 512], P('table'), may hold values from 1 to 100, as said below
Outputs:
- pooled: bfloat16 [4, 512, 128], P(None, ('table', 'row'))
The draws below stay inside these ranges and needn't reach their ends.
Inputs may be any that keep to these rules, and one draw needn't show every extreme that they name: `lengths`: the longest bag of each table has a power of two of at most 64 positions, or 100 positions, and some table has a bag of 100.
All inputs are finite; a program needn't handle non-finite values.
Results may differ from the reference program's by a relative error of at most 0.001.
Values may be sent and summed in bfloat16 or wider, within the bound.
A program may use at most 64 MiB of HBM per device.

```python
import math
import jax
import jax.numpy as jnp
import numpy as np
from jax import lax

D = 128
BAG = 100
NT = 4
ROWS = 524288
BATCH = 512


def draw_lengths(key, part):
    subkeys = jax.random.split(key, 4)
    exponent = jax.random.randint(subkeys[0], (NT, 1), 0, 8)
    table_caps = jnp.minimum(jnp.left_shift(jnp.ones_like(exponent), exponent), BAG)
    longest = jax.random.randint(subkeys[1], (), 0, NT)
    table_caps = jnp.where(jnp.arange(NT)[:, None] == longest, BAG, table_caps)
    uniform_draw = jax.random.randint(subkeys[2], (NT, BATCH), 0, 1 << 20)
    lengths = uniform_draw % table_caps + 1
    chosen = jax.random.randint(subkeys[3], (NT, 1), 0, BATCH)
    lengths = jnp.where(jnp.arange(BATCH)[None, :] == chosen, table_caps, lengths)
    return lengths.astype(jnp.int32)


def touch_ends(entries, key, least, largest):
    shape = entries.shape
    place = [jax.random.randint(jax.random.fold_in(key, axis), (), 0, shape[axis]) for axis in range(len(shape))]
    entries = entries.at[tuple(place)].set(least)
    longest = shape.index(max(shape))
    place[longest] = (place[longest] + 1) % shape[longest]
    return entries.at[tuple(place)].set(largest)


def block_scale(rng, extent, cuts, least, top_value):
    factor_of, own = 1.0, jax.random.fold_in(rng, 6)
    for dim, parts in cuts:
        heights = jnp.exp(jax.random.uniform(jax.random.fold_in(own, dim), (parts,), jnp.float32, least / len(cuts), top_value / len(cuts)))
        factor_of = factor_of * jnp.repeat(heights, extent[dim] // parts).reshape([-1 if axis == dim else 1 for axis in range(len(extent))])
    return factor_of


def wide_ids(own_key, dims, count, slope):
    loads = [min(1 << octave, count + 1 - (1 << octave)) * (1 << 20) // math.isqrt((1 << octave) ** slope) + 1 for octave in range((count + 1).bit_length()) if 1 << octave <= count]
    scale = 1 + sum(loads) // (1 << 30)
    grid = np.cumsum(np.array([max(1, weight // scale) for weight in loads]))
    lot = jax.random.randint(jax.random.fold_in(own_key, 1), dims, 0, int(grid[len(loads) - 1]))
    start = jnp.left_shift(1, jnp.searchsorted(jnp.asarray(grid, jnp.int32), lot, side="right").astype(jnp.int32))
    standing = start - 1 + jax.random.randint(jax.random.fold_in(own_key, 4), dims, 0, 1 << 30) % jnp.minimum(start, count + 1 - start)
    return jax.random.permutation(jax.random.fold_in(own_key, 2), count)[standing].astype(jnp.int32)


def noise(rng, shape, scale, most, cuts=(), kind=jnp.bfloat16):
    result = scale * jax.random.normal(rng, shape, jnp.float32)
    if cuts:
        result = result * block_scale(rng, shape, cuts, -0.22, 0.18)
    return jnp.clip(result, -most, most).astype(kind)


def setup_inputs(seed: int = 0) -> dict:
    key_list = jax.random.split(jax.random.key(seed), 5)
    return {
        "tables": noise(key_list[0], (NT, ROWS, D), 0.5, 3.0, ((0, 4), (1, 64))),
        "indices": touch_ends(wide_ids(key_list[1], (NT, BAG, BATCH), ROWS, 2), jax.random.fold_in(key_list[1], 3), 0, ROWS - 1).astype(jnp.int32),
        "weights": jnp.clip(0.19921875 + 0.80078125 * jax.random.uniform(key_list[2], (NT, BAG, BATCH), jnp.float32) ** block_scale(key_list[2], (NT, BAG, BATCH), ((0, 4),), -0.2, 0.2), 0.19921875, 1.0).astype(jnp.bfloat16),
        "lengths": draw_lengths(jax.random.fold_in(key_list[4], 71), 0),
    }


bag_block = 10


def pool_table(operands):
    table_rows, index_rows, weight, length = operands
    position = jnp.arange(BAG, dtype=jnp.int32)[:, None]
    factors = jnp.where(position < length[None, :], weight, jnp.zeros_like(weight))

    def add_block(running, first_row):
        index_block = lax.dynamic_slice_in_dim(index_rows, first_row, bag_block, 0)
        factor_block = lax.dynamic_slice_in_dim(factors, first_row, bag_block, 0)
        gathered = jnp.take(table_rows, index_block, axis=0)
        running = running + jnp.einsum("lb,lbd->bd", factor_block.astype(jnp.float32), gathered.astype(jnp.float32))
        return running, None

    starts = jnp.arange(0, BAG, bag_block, dtype=jnp.int32)
    running, unused = lax.scan(add_block, jnp.zeros((BATCH, D), jnp.float32), starts)
    return running.astype(jnp.bfloat16)


def reference(tables, indices, weights, lengths):
    return lax.map(pool_table, (tables, indices, weights, lengths))
```

```python
import functools

import jax
import jax.numpy as jnp
from jax import lax
from jax.experimental import pallas as pl
from jax.experimental.pallas import tpu as pltpu
from jax.sharding import PartitionSpec as P

MESH = pl.DeviceIdType.MESH
LANES = 128
BLOCK = 8
PAIR = 2
F32 = jnp.float32
BF16 = jnp.bfloat16
I32 = jnp.int32


def pool_kernel(
    t_hbm, i_hbm, w_hbm, l_hbm, out_ref,
    t_bf, t_f32, idx_ref, wt_ref, len_ref, pos_ref, val_ref, slot_ref, rows_ref, slot_smem,
    t_sem, in_sem, smem_sem,
):
    rows, width = t_f32.shape
    bag, batch = idx_ref.shape
    padded = pos_ref.shape[0]
    tiles = batch // LANES
    chunks = t_sem.shape[0]
    chunk = rows // chunks

    def table_copy(c):
        part = pl.ds(c * chunk, chunk)
        return pltpu.make_async_copy(t_hbm.at[0, part], t_bf.at[part], t_sem.at[c])

    copies = [
        pltpu.make_async_copy(i_hbm.at[0], idx_ref, in_sem.at[0]),
        pltpu.make_async_copy(w_hbm.at[0], wt_ref, in_sem.at[1]),
        pltpu.make_async_copy(l_hbm, len_ref, in_sem.at[2]),
    ]
    for copy in copies:
        copy.start()
    for c in range(chunks):
        table_copy(c).start()
    out_ref[...] = jnp.zeros_like(out_ref)
    for copy in copies:
        copy.wait()

    local = idx_ref[...] - lax.axis_index("row") * rows
    position = lax.broadcasted_iota(I32, (bag, batch), 0)
    inside = (local >= 0) & (local < rows) & (position < len_ref[0:1, :])
    ones = jnp.where(inside, 1.0, 0.0)
    lower = lax.broadcasted_iota(I32, (bag, bag), 0) >= lax.broadcasted_iota(I32, (bag, bag), 1)
    count = jnp.dot(
        jnp.where(lower, 1.0, 0.0).astype(BF16), ones.astype(BF16), preferred_element_type=F32
    )
    milli = (wt_ref[...].astype(F32) * 1024.0).astype(I32)
    base = jnp.zeros((1, LANES), F32)
    pos_ref[bag:padded, :] = jnp.full((padded - bag, batch), -1, I32)
    val_ref[bag:padded, :] = jnp.zeros((padded - bag, batch), I32)
    for tile in range(tiles):
        lanes = slice(tile * LANES, (tile + 1) * LANES)
        rank = count[:, lanes] + (base - 1.0)
        pos_ref[:bag, lanes] = jnp.where(inside[:, lanes], rank, -1.0).astype(I32)
        val_ref[:bag, lanes] = local[:, lanes] + milli[:, lanes] * 32768 + tile * 8192
        base = base + count[bag - 1 : bag, lanes]
    slot_rows = jnp.max(base).astype(I32)

    for c in range(chunks):
        table_copy(c).wait()
        t_f32[c * chunk : (c + 1) * chunk, :] = t_bf[c * chunk : (c + 1) * chunk, :].astype(F32)

    def smem_copy(slot):
        return pltpu.make_async_copy(rows_ref.at[slot], slot_smem.at[slot], smem_sem.at[slot])

    def select(block, slot):
        first = block * BLOCK
        totals = [jnp.zeros((8, LANES), I32) for _ in range(BLOCK)]
        for tile in range(tiles):
            lanes = slice(tile * LANES, (tile + 1) * LANES)
            for r in range(padded // 8):
                here = pos_ref[r * 8 : r * 8 + 8, lanes] - first
                value = val_ref[r * 8 : r * 8 + 8, lanes]
                for k in range(BLOCK):
                    totals[k] = totals[k] + jnp.where(here == k, value, 0)
        packed = jnp.concatenate([t.sum(axis=0, keepdims=True) for t in totals], axis=0)
        slot_ref[slot] = packed
        rows_ref[slot] = packed & 8191
        smem_copy(slot).start()

    blocks = (slot_rows + (BLOCK - 1)) // BLOCK

    @pl.when(blocks > 0)
    def _():
        select(0, 0)

    lane = lax.broadcasted_iota(I32, (1, LANES), 1)
    lane_place = ((lane >> 1) & 31) * 16 + (lane >> 6) * 2 + (lane & 1)
    bag_place = lax.broadcasted_iota(I32, (batch, PAIR * LANES), 0)

    def process(gathered, block, slot):
        pairs = (jnp.minimum(slot_rows - block * BLOCK, BLOCK) + (PAIR - 1)) // PAIR

        @pl.loop(0, pairs)
        def _(pair):
            for k in range(PAIR):
                row = pair * PAIR + k

                @pl.loop(0, LANES, step=32)
                def _(start):
                    for u in range(32):
                        source = slot_smem[slot, row, start + u]
                        gathered[pl.ds(k * LANES + start + u, 1), :] = t_f32[pl.ds(source, 1), :]

            parts = []
            for k in range(PAIR):
                packed = slot_ref[slot, pl.ds(pair * PAIR + k, 1), :]
                place = lane_place + ((packed >> 13) & 3) * 4
                weight = (packed >> 15).astype(F32) * (1.0 / 1024.0)
                parts.append((place, weight))
            place = jnp.concatenate([p[0] for p in parts], axis=1)
            weight = jnp.concatenate([p[1] for p in parts], axis=1)
            select_bags = jnp.where(bag_place == place, weight, 0.0).astype(BF16)
            out_ref[...] += jnp.dot(
                select_bags, gathered[...].astype(BF16), preferred_element_type=F32
            )

    def work(gathered):
        @pl.loop(0, blocks)
        def _(block):
            slot = lax.rem(block, 2)

            @pl.when(block + 1 < blocks)
            def _():
                select(block + 1, 1 - slot)

            smem_copy(slot).wait()
            process(gathered, block, slot)

    pl.run_scoped(work, pltpu.VMEM((PAIR * LANES, width), F32))


def pool(tables, indices, weights, lengths):
    rows, width = tables.shape[1:]
    bag, batch = indices.shape[1:]
    padded = (bag + 7) // 8 * 8
    return pl.pallas_call(
        pool_kernel,
        out_shape=jax.ShapeDtypeStruct((batch, width), F32),
        in_specs=[pl.BlockSpec(memory_space=pl.ANY)] * 4,
        out_specs=pl.BlockSpec(memory_space=pltpu.VMEM),
        scratch_shapes=[
            pltpu.VMEM((rows, width), BF16),
            pltpu.VMEM((rows, width), F32),
            pltpu.VMEM((bag, batch), I32),
            pltpu.VMEM((bag, batch), BF16),
            pltpu.VMEM((1, batch), I32),
            pltpu.VMEM((padded, batch), I32),
            pltpu.VMEM((padded, batch), I32),
            pltpu.VMEM((2, BLOCK, LANES), I32),
            pltpu.VMEM((2, BLOCK, LANES), I32),
            pltpu.SMEM((2, BLOCK, LANES), I32),
            pltpu.SemaphoreType.DMA((4,)),
            pltpu.SemaphoreType.DMA((3,)),
            pltpu.SemaphoreType.DMA((2,)),
        ],
        compiler_params=pltpu.CompilerParams(vmem_limit_bytes=24 * 1024 * 1024),
        name="pool",
    )(tables, indices, weights, lengths)


def exchange_kernel(tables, p_ref, out_ref, recv1, send2, recv2, s1_send, s1_recv, s2_send, s2_recv):
    groups = recv1.shape[0]
    ends = recv2.shape[0]
    high = ends // tables
    table, row = lax.axis_index("table"), lax.axis_index("row")
    plane, place = row // groups, lax.rem(row, groups)
    part = recv1.shape[1]

    def plane_peer(d):
        return lax.rem(place + d, groups)

    def line_peer(d):
        return lax.rem(table + d // high, tables), lax.rem(plane + d % high, high)

    barrier = pltpu.get_barrier_semaphore()
    for d in range(1, groups):
        pl.semaphore_signal(
            barrier, inc=1, device_id=(table, plane * groups + plane_peer(d)), device_id_type=MESH
        )
    for d in range(1, ends):
        t, h = line_peer(d)
        pl.semaphore_signal(barrier, inc=1, device_id=(t, h * groups + place), device_id_type=MESH)
    pl.semaphore_wait(barrier, groups + ends - 2)

    def first_copy(d):
        peer = plane_peer(d)
        return pltpu.make_async_remote_copy(
            src_ref=p_ref.at[peer],
            dst_ref=recv1.at[d],
            send_sem=s1_send.at[d],
            recv_sem=s1_recv.at[d],
            device_id=(table, plane * groups + peer),
            device_id_type=MESH,
        )

    for d in range(1, groups):
        first_copy(d).start()
    total = p_ref[place]
    for d in range(1, groups):
        first_copy(d).wait_recv()
        total = total + recv1[d]
    each = part // ends
    for q in range(ends):
        send2[q] = total[q * each : (q + 1) * each, :]

    def second_copy(d):
        t, h = line_peer(d)
        return pltpu.make_async_remote_copy(
            src_ref=send2.at[t * high + h],
            dst_ref=recv2.at[d],
            send_sem=s2_send.at[d],
            recv_sem=s2_recv.at[d],
            device_id=(t, h * groups + place),
            device_id_type=MESH,
        )

    for d in range(1, ends):
        second_copy(d).start()
    recv2[0] = send2[table * high + plane]
    for d in range(1, ends):
        second_copy(d).wait_recv()
    for dt in range(tables):
        source = lax.rem(table - dt + tables, tables)
        value = recv2[dt * high]
        for dh in range(1, high):
            value = value + recv2[dt * high + dh]
        out_ref[source] = value.astype(BF16)
    for d in range(1, groups):
        first_copy(d).wait_send()
    for d in range(1, ends):
        second_copy(d).wait_send()


def exchange(partial, tables, groups, ends):
    batch, width = partial.shape
    part = batch // groups
    each = part // ends
    return pl.pallas_call(
        functools.partial(exchange_kernel, tables),
        out_shape=jax.ShapeDtypeStruct((tables, each, width), BF16),
        in_specs=[pl.BlockSpec(memory_space=pltpu.VMEM)],
        out_specs=pl.BlockSpec(memory_space=pltpu.VMEM),
        scratch_shapes=[
            pltpu.VMEM((groups, part, width), F32),
            pltpu.VMEM((ends, each, width), F32),
            pltpu.VMEM((ends, each, width), F32),
            pltpu.SemaphoreType.DMA((groups,)),
            pltpu.SemaphoreType.DMA((groups,)),
            pltpu.SemaphoreType.DMA((ends,)),
            pltpu.SemaphoreType.DMA((ends,)),
        ],
        compiler_params=pltpu.CompilerParams(
            collective_id=0, has_side_effects=True, vmem_limit_bytes=24 * 1024 * 1024
        ),
        name="exchange",
    )(partial.reshape(groups, part, width))


def on_device(tables, indices, weights, lengths):
    partial = pool(tables, indices, weights, lengths)
    return exchange(partial, lax.axis_size("table"), 32, 8)


def solution(mesh):
    placed = (
        P("table", "row", None),
        P("table", None, None),
        P("table", None, None),
        P("table", None),
    )
    return jax.shard_map(
        on_device,
        mesh=mesh,
        in_specs=placed,
        out_specs=P(None, ("table", "row"), None),
        check_vma=False,
    )
```

```python
import functools

import jax
import jax.numpy as jnp
from jax import lax
from jax.experimental import pallas as pl
from jax.experimental.pallas import tpu as pltpu
from jax.sharding import PartitionSpec as P

MESH = pl.DeviceIdType.MESH
LANES = 128
BLOCK = 8
PAIR = 2
VOTERS = 3
F32 = jnp.float32
BF16 = jnp.bfloat16
I32 = jnp.int32


def pool_kernel(
    t_hbm, i_hbm, w_hbm, l_hbm, out_ref,
    t_bf, t_f32, idx_ref, wt_ref, len_ref, pos_ref, val_ref, slot_ref, rows_ref, gathered, slot_smem,
    t_sem, in_sem, smem_sem,
):
    rows, width = t_f32.shape
    bag, batch = wt_ref.shape
    padded = pos_ref.shape[0]
    tiles = batch // LANES
    chunks = t_sem.shape[0]
    chunk = rows // chunks

    def table_copy(c):
        part = pl.ds(c * chunk, chunk)
        return pltpu.make_async_copy(t_hbm.at[0, part], t_bf.at[part], t_sem.at[c])

    copies = [
        pltpu.make_async_copy(i_hbm, idx_ref, in_sem.at[0]),
        pltpu.make_async_copy(w_hbm.at[0], wt_ref, in_sem.at[1]),
        pltpu.make_async_copy(l_hbm, len_ref, in_sem.at[2]),
    ]
    for copy in copies:
        copy.start()
    for c in range(chunks):
        table_copy(c).start()
    pos_ref[bag:padded, :] = jnp.full((padded - bag, batch), -1, I32)
    val_ref[bag:padded, :] = jnp.zeros((padded - bag, batch), I32)
    for copy in copies:
        copy.wait()

    first_row = lax.axis_index("row") * rows
    position = lax.broadcasted_iota(I32, (bag, LANES), 0)
    lane_tiles = [slice(tile * LANES, (tile + 1) * LANES) for tile in range(tiles)]
    locals_, insides = [], []
    for tile, lanes in enumerate(lane_tiles):
        local = idx_ref[pl.ds(tile, bag, stride=tiles), :] - first_row
        inside = (local >= 0) & (local < rows) & (position < len_ref[0:1, lanes])
        locals_.append(local)
        insides.append(inside)

    bits = (rows - 1).bit_length()
    votes = [jnp.zeros((8, LANES), I32) for _ in range(bits + 1)]
    for local, inside in zip(locals_, insides):
        for r in range(VOTERS):
            part = slice(r * 8, r * 8 + 8)
            ballot = jnp.where(inside[part], local[part] + rows, 0)
            for b in range(bits + 1):
                votes[b] = votes[b] + ((ballot >> b) & 1)
    tally = jnp.dot(
        jnp.concatenate(votes, axis=0).astype(F32).astype(BF16),
        jnp.ones((LANES, LANES), BF16),
        preferred_element_type=F32,
    ).reshape(bits + 1, 8, LANES).sum(axis=1)
    leader = jnp.zeros((1, LANES), I32)
    for b in range(bits):
        leader = leader + jnp.where(2.0 * tally[b : b + 1] > tally[bits : bits + 1], 1 << b, 0)

    lower = lax.broadcasted_iota(I32, (bag, bag), 0) >= lax.broadcasted_iota(I32, (bag, bag), 1)
    lower = jnp.where(lower, 1.0, 0.0).astype(BF16)
    base = jnp.zeros((1, LANES), F32)
    lead_weights = []
    for tile, lanes in enumerate(lane_tiles):
        local, inside = locals_[tile], insides[tile]
        weight = wt_ref[:, lanes].astype(F32)
        leads = inside & (local == leader)
        lead_weights.append(jnp.where(leads, weight, 0.0).sum(axis=0, keepdims=True))
        inside = inside & (local != leader)
        ones = jnp.where(inside, 1.0, 0.0).astype(BF16)
        count = jnp.dot(lower, ones, preferred_element_type=F32)
        pos_ref[:bag, lanes] = jnp.where(inside, count + (base - 1.0), -1.0).astype(I32)
        milli = (weight * 1024.0).astype(I32)
        val_ref[:bag, lanes] = local + milli * 32768 + tile * 8192
        base = base + count[bag - 1 : bag, :]
    slot_rows = jnp.max(base).astype(I32)
    lead_row = jnp.max(leader)
    lead_columns = jnp.concatenate(lead_weights + [jnp.zeros((8 - tiles, LANES), F32)], axis=0).T

    def smem_copy(slot):
        return pltpu.make_async_copy(rows_ref.at[slot], slot_smem.at[slot], smem_sem.at[slot])

    def select(block, slot):
        first = block * BLOCK
        totals = [jnp.zeros((8, LANES), I32) for _ in range(BLOCK)]
        for lanes in lane_tiles:
            for r in range(padded // 8):
                here = pos_ref[r * 8 : r * 8 + 8, lanes] - first
                value = val_ref[r * 8 : r * 8 + 8, lanes]
                for k in range(BLOCK):
                    totals[k] = totals[k] + jnp.where(here == k, value, 0)
        packed = jnp.concatenate([t.sum(axis=0, keepdims=True) for t in totals], axis=0)
        slot_ref[slot] = packed
        rows_ref[slot] = packed & 8191
        smem_copy(slot).start()

    blocks = (slot_rows + (BLOCK - 1)) // BLOCK

    @pl.when(blocks > 0)
    def _():
        select(0, 0)

    for c in range(chunks):
        table_copy(c).wait()
        t_f32[c * chunk : (c + 1) * chunk, :] = t_bf[c * chunk : (c + 1) * chunk, :].astype(F32)
    lead_values = t_f32[pl.ds(lead_row, 1), :]
    for tile, lanes in enumerate(lane_tiles):
        out_ref[lanes, :] = lead_columns[:, tile : tile + 1] * lead_values

    diagonal = lax.broadcasted_iota(I32, (LANES, LANES), 0) == lax.broadcasted_iota(
        I32, (LANES, LANES), 1
    )

    @pl.loop(0, blocks)
    def _(block):
        slot = lax.rem(block, 2)

        @pl.when(block + 1 < blocks)
        def _():
            select(block + 1, 1 - slot)

        smem_copy(slot).wait()
        pairs = (jnp.minimum(slot_rows - block * BLOCK, BLOCK) + (PAIR - 1)) // PAIR

        @pl.loop(0, pairs)
        def _(pair):
            packed = []
            for k in range(PAIR):
                row = pair * PAIR + k
                for u in range(LANES):
                    source = slot_smem[slot, row, u]
                    gathered[k * LANES + u : k * LANES + u + 1, :] = t_f32[pl.ds(source, 1), :]
                packed.append(slot_ref[slot, pl.ds(row, 1), :])
            values = gathered[...].astype(BF16)
            for tile, lanes in enumerate(lane_tiles):
                parts = []
                for p in packed:
                    weight = (p >> 15).astype(F32) * (1.0 / 1024.0)
                    weight = jnp.where(((p >> 13) & 3) == tile, weight, 0.0)
                    parts.append(jnp.where(diagonal, weight, 0.0).astype(BF16))
                out_ref[lanes, :] += jnp.dot(
                    jnp.concatenate(parts, axis=1), values, preferred_element_type=F32
                )


def pool(tables, indices, weights, lengths):
    rows, width = tables.shape[1:]
    bag, batch = indices.shape[1:]
    padded = (bag + 7) // 8 * 8
    tiles = batch // LANES
    return pl.pallas_call(
        pool_kernel,
        out_shape=jax.ShapeDtypeStruct((batch, width), F32),
        in_specs=[pl.BlockSpec(memory_space=pltpu.HBM)] * 4,
        out_specs=pl.BlockSpec(memory_space=pltpu.VMEM),
        scratch_shapes=[
            pltpu.VMEM((rows, width), BF16),
            pltpu.VMEM((rows, width), F32),
            pltpu.VMEM((bag * tiles, LANES), I32),
            pltpu.VMEM((bag, batch), BF16),
            pltpu.VMEM((1, batch), I32),
            pltpu.VMEM((padded, batch), I32),
            pltpu.VMEM((padded, batch), I32),
            pltpu.VMEM((2, BLOCK, LANES), I32),
            pltpu.VMEM((2, BLOCK, LANES), I32),
            pltpu.VMEM((PAIR * LANES, width), F32),
            pltpu.SMEM((2, BLOCK, LANES), I32),
            pltpu.SemaphoreType.DMA((4,)),
            pltpu.SemaphoreType.DMA((3,)),
            pltpu.SemaphoreType.DMA((2,)),
        ],
        compiler_params=pltpu.CompilerParams(vmem_limit_bytes=24 * 1024 * 1024),
        name="pool",
    )(tables, pltpu.with_memory_space_constraint(indices.reshape(bag * tiles, LANES), pltpu.HBM), weights, lengths)


def exchange_kernel(tables, p_ref, out_ref, recv1, send2, recv2, s1_send, s1_recv, s2_send, s2_recv):
    groups = recv1.shape[0]
    ends = recv2.shape[0]
    high = ends // tables
    table, row = lax.axis_index("table"), lax.axis_index("row")
    plane, place = row // groups, lax.rem(row, groups)

    def plane_peer(d):
        return lax.rem(place + d, groups)

    def line_peer(d):
        return lax.rem(table + d // high, tables), lax.rem(plane + d % high, high)

    barrier = pltpu.get_barrier_semaphore()
    for d in range(1, groups):
        pl.semaphore_signal(
            barrier, inc=1, device_id=(table, plane * groups + plane_peer(d)), device_id_type=MESH
        )
    for d in range(1, ends):
        t, h = line_peer(d)
        pl.semaphore_signal(barrier, inc=1, device_id=(t, h * groups + place), device_id_type=MESH)
    pl.semaphore_wait(barrier, groups + ends - 2)

    def first_copy(d):
        peer = plane_peer(d)
        return pltpu.make_async_remote_copy(
            src_ref=p_ref.at[:, peer],
            dst_ref=recv1.at[d],
            send_sem=s1_send.at[d],
            recv_sem=s1_recv.at[d],
            device_id=(table, plane * groups + peer),
            device_id_type=MESH,
        )

    for d in range(1, groups):
        first_copy(d).start()
    total = p_ref[:, place]
    for d in range(1, groups):
        first_copy(d).wait_recv()
        total = total + recv1[d]
    send2[...] = total

    def second_copy(d):
        t, h = line_peer(d)
        return pltpu.make_async_remote_copy(
            src_ref=send2.at[t * high + h],
            dst_ref=recv2.at[d],
            send_sem=s2_send.at[d],
            recv_sem=s2_recv.at[d],
            device_id=(t, h * groups + place),
            device_id_type=MESH,
        )

    for d in range(1, ends):
        second_copy(d).start()
    recv2[0] = send2[table * high + plane]
    for d in range(1, ends):
        second_copy(d).wait_recv()
    for dt in range(tables):
        source = lax.rem(table - dt + tables, tables)
        value = recv2[dt * high]
        for dh in range(1, high):
            value = value + recv2[dt * high + dh]
        out_ref[source] = value.astype(BF16)
    for d in range(1, groups):
        first_copy(d).wait_send()
    for d in range(1, ends):
        second_copy(d).wait_send()


def exchange(partial, tables, groups, ends):
    batch, width = partial.shape
    each = batch // (groups * ends)
    return pl.pallas_call(
        functools.partial(exchange_kernel, tables),
        out_shape=jax.ShapeDtypeStruct((tables, each, width), BF16),
        in_specs=[pl.BlockSpec(memory_space=pltpu.VMEM)],
        out_specs=pl.BlockSpec(memory_space=pltpu.VMEM),
        scratch_shapes=[
            pltpu.VMEM((groups, ends, each, width), F32),
            pltpu.VMEM((ends, each, width), F32),
            pltpu.VMEM((ends, each, width), F32),
            pltpu.SemaphoreType.DMA((groups,)),
            pltpu.SemaphoreType.DMA((groups,)),
            pltpu.SemaphoreType.DMA((ends,)),
            pltpu.SemaphoreType.DMA((ends,)),
        ],
        compiler_params=pltpu.CompilerParams(
            collective_id=0, has_side_effects=True, vmem_limit_bytes=24 * 1024 * 1024
        ),
        name="exchange",
    )(partial.reshape(ends, groups, each, width))


def on_device(tables, indices, weights, lengths):
    tables, weights, lengths = [pltpu.with_memory_space_constraint(x, pltpu.HBM) for x in (tables, weights, lengths)]
    partial = pool(tables, indices, weights, lengths)
    return exchange(partial, lax.axis_size("table"), 32, 8)


def solution(mesh):
    placed = (
        P("table", "row", None),
        P("table", None, None),
        P("table", None, None),
        P("table", None),
    )
    return jax.shard_map(
        on_device,
        mesh=mesh,
        in_specs=placed,
        out_specs=P(None, ("table", "row"), None),
        check_vma=False,
    )
```

```python
import functools

import jax
import jax.numpy as jnp
from jax import lax
from jax.experimental import pallas as pl
from jax.experimental.pallas import tpu as pltpu
from jax.sharding import PartitionSpec as P

MESH = pl.DeviceIdType.MESH
LANES = 128
BLOCK = 8
KEEP = 16
PAIR = 2
UNROLL = 256
VOTERS = 3
F32 = jnp.float32
BF16 = jnp.bfloat16
I32 = jnp.int32


def bag_places(batch):
    lane = lax.broadcasted_iota(I32, (1, LANES), 1)
    return ((lane >> 1) & 31) * 16 + (lane >> 6) * 2 + (lane & 1)


def pick_bags(packed, batch):
    lane_place = bag_places(batch)
    place = jnp.concatenate([lane_place + ((p >> 13) & 3) * 4 for p in packed], axis=1)
    weight = jnp.concatenate([(p >> 15).astype(F32) * (1.0 / 1024.0) for p in packed], axis=1)
    rows = lax.broadcasted_iota(I32, (batch, place.shape[1]), 0)
    return jnp.where(rows == place, weight, 0.0).astype(BF16)


def rank_kernel(
    t_hbm, i_hbm, w_hbm, l_hbm, keep_ref, ids_ref, lead_ref, over_ref,
    t_bf, t_f32, idx_ref, wt_ref, len_ref, pos_ref, val_ref, slot_ref, rows_ref, gathered, slot_smem,
    t_sem, in_sem, smem_sem,
):
    rows, width = t_f32.shape
    bag, batch = wt_ref.shape
    padded = pos_ref.shape[0]
    tiles = batch // LANES

    copies = [
        pltpu.make_async_copy(i_hbm, idx_ref, in_sem.at[0]),
        pltpu.make_async_copy(w_hbm.at[0], wt_ref, in_sem.at[1]),
        pltpu.make_async_copy(l_hbm, len_ref, in_sem.at[2]),
    ]
    for copy in copies:
        copy.start()
    pos_ref[bag:padded, :] = jnp.full((padded - bag, batch), -1, I32)
    val_ref[bag:padded, :] = jnp.zeros((padded - bag, batch), I32)
    over_ref[...] = jnp.zeros_like(over_ref)
    for copy in copies:
        copy.wait()

    first_row = lax.axis_index("row") * rows
    position = lax.broadcasted_iota(I32, (bag, LANES), 0)
    lane_tiles = [slice(tile * LANES, (tile + 1) * LANES) for tile in range(tiles)]
    locals_, insides = [], []
    for tile, lanes in enumerate(lane_tiles):
        local = idx_ref[pl.ds(tile, bag, stride=tiles), :] - first_row
        inside = (local >= 0) & (local < rows) & (position < len_ref[0:1, lanes])
        locals_.append(local)
        insides.append(inside)

    bits = (rows - 1).bit_length()
    votes = [jnp.zeros((8, LANES), I32) for _ in range(bits + 1)]
    for local, inside in zip(locals_, insides):
        for r in range(VOTERS):
            part = slice(r * 8, r * 8 + 8)
            ballot = jnp.where(inside[part], local[part] + rows, 0)
            for b in range(bits + 1):
                votes[b] = votes[b] + ((ballot >> b) & 1)
    tally = jnp.dot(
        jnp.concatenate(votes, axis=0).astype(F32).astype(BF16),
        jnp.ones((LANES, LANES), BF16),
        preferred_element_type=F32,
    ).reshape(bits + 1, 8, LANES).sum(axis=1)
    leader = jnp.zeros((1, LANES), I32)
    for b in range(bits):
        leader = leader + jnp.where(2.0 * tally[b : b + 1] > tally[bits : bits + 1], 1 << b, 0)

    lower = lax.broadcasted_iota(I32, (bag, bag), 0) >= lax.broadcasted_iota(I32, (bag, bag), 1)
    lower = jnp.where(lower, 1.0, 0.0).astype(BF16)
    base = jnp.zeros((1, LANES), F32)
    for tile, lanes in enumerate(lane_tiles):
        local, inside = locals_[tile], insides[tile]
        weight = wt_ref[:, lanes].astype(F32)
        leads = inside & (local == leader)
        lead_ref[tile : tile + 1, :] = jnp.where(leads, weight, 0.0).sum(axis=0, keepdims=True)
        inside = inside & (local != leader)
        ones = jnp.where(inside, 1.0, 0.0).astype(BF16)
        count = jnp.dot(lower, ones, preferred_element_type=F32)
        pos_ref[:bag, lanes] = jnp.where(inside, count + (base - 1.0), -1.0).astype(I32)
        milli = (weight * 1024.0).astype(I32)
        val_ref[:bag, lanes] = local + milli * 32768 + tile * 8192
        base = base + count[bag - 1 : bag, :]
    lead_ref[tiles:, :] = jnp.zeros((8 - tiles, LANES), F32)
    ids_ref[KEEP : KEEP + 8, :] = jnp.broadcast_to(leader, (8, LANES))

    def chosen(first):
        totals = [jnp.zeros((8, LANES), I32) for _ in range(BLOCK)]
        for lanes in lane_tiles:
            for r in range(padded // 8):
                here = pos_ref[r * 8 : r * 8 + 8, lanes] - first
                value = val_ref[r * 8 : r * 8 + 8, lanes]
                for k in range(BLOCK):
                    totals[k] = totals[k] + jnp.where(here == k, value, 0)
        return jnp.concatenate([t.sum(axis=0, keepdims=True) for t in totals], axis=0)

    for first in range(0, KEEP, BLOCK):
        packed = chosen(first)
        keep_ref[first : first + BLOCK, :] = packed
        ids_ref[first : first + BLOCK, :] = packed & 8191

    slot_rows = jnp.max(base).astype(I32) - KEEP

    @pl.when(slot_rows > 0)
    def _():
        table_copy = pltpu.make_async_copy(t_hbm.at[0], t_bf, t_sem)
        table_copy.start()

        def smem_copy(slot):
            return pltpu.make_async_copy(rows_ref.at[slot], slot_smem.at[slot], smem_sem.at[slot])

        def select(block, slot):
            packed = chosen(KEEP + block * BLOCK)
            slot_ref[slot] = packed
            rows_ref[slot] = packed & 8191
            smem_copy(slot).start()

        blocks = (slot_rows + (BLOCK - 1)) // BLOCK
        select(0, 0)
        table_copy.wait()

        @pl.loop(0, rows, step=512)
        def _(row):
            t_f32[pl.ds(row, 512), :] = t_bf[pl.ds(row, 512), :].astype(F32)

        @pl.loop(0, blocks)
        def _(block):
            slot = lax.rem(block, 2)

            @pl.when(block + 1 < blocks)
            def _():
                select(block + 1, 1 - slot)

            smem_copy(slot).wait()
            pairs = (jnp.minimum(slot_rows - block * BLOCK, BLOCK) + (PAIR - 1)) // PAIR

            @pl.loop(0, pairs)
            def _(pair):
                packed = []
                for k in range(PAIR):
                    row = pair * PAIR + k
                    for u in range(LANES):
                        source = slot_smem[slot, row, u]
                        gathered[k * LANES + u : k * LANES + u + 1, :] = t_f32[pl.ds(source, 1), :]
                    packed.append(slot_ref[slot, pl.ds(row, 1), :])
                over_ref[...] += jnp.dot(
                    pick_bags(packed, batch),
                    gathered[...].astype(BF16),
                    preferred_element_type=F32,
                )


def rank(tables, indices, weights, lengths):
    rows, width = tables.shape[1:]
    bag, batch = indices.shape[1:]
    padded = (bag + 7) // 8 * 8
    tiles = batch // LANES
    operands = (tables, indices.reshape(bag * tiles, LANES), weights, lengths)
    return pl.pallas_call(
        rank_kernel,
        out_shape=(
            jax.ShapeDtypeStruct((KEEP, LANES), I32),
            jax.ShapeDtypeStruct((KEEP + 8, LANES), I32),
            jax.ShapeDtypeStruct((8, LANES), F32),
            jax.ShapeDtypeStruct((batch, width), F32),
        ),
        in_specs=[pl.BlockSpec(memory_space=pltpu.HBM)] * 4,
        out_specs=(pl.BlockSpec(memory_space=pltpu.VMEM),) * 4,
        scratch_shapes=[
            pltpu.VMEM((rows, width), BF16),
            pltpu.VMEM((rows, width), F32),
            pltpu.VMEM((bag * tiles, LANES), I32),
            pltpu.VMEM((bag, batch), BF16),
            pltpu.VMEM((1, batch), I32),
            pltpu.VMEM((padded, batch), I32),
            pltpu.VMEM((padded, batch), I32),
            pltpu.VMEM((2, BLOCK, LANES), I32),
            pltpu.VMEM((2, BLOCK, LANES), I32),
            pltpu.VMEM((PAIR * LANES, width), F32),
            pltpu.SMEM((2, BLOCK, LANES), I32),
            pltpu.SemaphoreType.DMA,
            pltpu.SemaphoreType.DMA((3,)),
            pltpu.SemaphoreType.DMA((2,)),
        ],
        compiler_params=pltpu.CompilerParams(vmem_limit_bytes=24 * 1024 * 1024),
        name="rank",
    )(*[pltpu.with_memory_space_constraint(x, pltpu.HBM) for x in operands])


def exchange_kernel(
    tables, t_hbm, keep_ref, ids_ref, lead_ref, over_ref, out_ref,
    t_bf, t_f32, gathered, pool, recv1, send2, recv2, ids_smem,
    t_sem, ids_sem, s1_send, s1_recv, s2_send, s2_recv,
):
    groups, part, width = recv1.shape
    ends, each = recv2.shape[:2]
    high = ends // tables
    batch = pool.shape[0]
    rows = t_f32.shape[0]
    chunks = t_sem.shape[0]
    chunk = rows // chunks
    table, row = lax.axis_index("table"), lax.axis_index("row")
    plane, place = row // groups, lax.rem(row, groups)

    def table_copy(c):
        span = pl.ds(c * chunk, chunk)
        return pltpu.make_async_copy(t_hbm.at[0, span], t_bf.at[span], t_sem.at[c])

    ids_copy = pltpu.make_async_copy(ids_ref, ids_smem, ids_sem)
    ids_copy.start()
    for c in range(chunks):
        table_copy(c).start()

    def plane_peer(d):
        return lax.rem(place + d, groups)

    def line_peer(d):
        return lax.rem(table + d // high, tables), lax.rem(plane + d % high, high)

    barrier = pltpu.get_barrier_semaphore()
    for d in range(1, groups):
        pl.semaphore_signal(
            barrier, inc=1, device_id=(table, plane * groups + plane_peer(d)), device_id_type=MESH
        )
    for d in range(1, ends):
        t, h = line_peer(d)
        pl.semaphore_signal(barrier, inc=1, device_id=(t, h * groups + place), device_id_type=MESH)

    bag_rows = lax.broadcasted_iota(I32, (batch, LANES), 0)
    lead = jnp.zeros((batch, LANES), F32)
    for tile in range(batch // LANES):
        lead = lead + jnp.where(
            bag_rows == bag_places(batch) + tile * 4, lead_ref[tile : tile + 1, :], 0.0
        )
    lead = lead.sum(axis=1, keepdims=True)

    for c in range(chunks):
        table_copy(c).wait()
        t_f32[c * chunk : (c + 1) * chunk, :] = t_bf[c * chunk : (c + 1) * chunk, :].astype(F32)
    ids_copy.wait()
    pool[...] = over_ref[...] + lead * t_f32[pl.ds(ids_smem[KEEP, 0], 1), :]
    for first in range(0, KEEP, PAIR):

        @pl.loop(0, PAIR * LANES, unroll=UNROLL)
        def _(u):
            source = ids_smem[first + u // LANES, u % LANES]
            gathered[pl.ds(first * LANES + u, 1), :] = t_f32[pl.ds(source, 1), :]

        pool[...] += jnp.dot(
            pick_bags([keep_ref[first + k : first + k + 1, :] for k in range(PAIR)], batch),
            gathered[first * LANES : (first + PAIR) * LANES, :].astype(BF16),
            preferred_element_type=F32,
        )

    pl.semaphore_wait(barrier, groups + ends - 2)

    def first_copy(d):
        peer = plane_peer(d)
        return pltpu.make_async_remote_copy(
            src_ref=pool.at[pl.ds(pl.multiple_of(peer * part, part), part)],
            dst_ref=recv1.at[d],
            send_sem=s1_send.at[d],
            recv_sem=s1_recv.at[d],
            device_id=(table, plane * groups + peer),
            device_id_type=MESH,
        )

    for d in range(1, groups):
        first_copy(d).start()
    total = pool[pl.ds(pl.multiple_of(place * part, part), part), :]
    for d in range(1, groups):
        first_copy(d).wait_recv()
        total = total + recv1[d]
    for q in range(ends):
        send2[q] = total[q * each : (q + 1) * each, :]

    def second_copy(d):
        t, h = line_peer(d)
        return pltpu.make_async_remote_copy(
            src_ref=send2.at[t * high + h],
            dst_ref=recv2.at[d],
            send_sem=s2_send.at[d],
            recv_sem=s2_recv.at[d],
            device_id=(t, h * groups + place),
            device_id_type=MESH,
        )

    for d in range(1, ends):
        second_copy(d).start()
    recv2[0] = send2[table * high + plane]
    for d in range(1, ends):
        second_copy(d).wait_recv()
    for dt in range(tables):
        source = lax.rem(table - dt + tables, tables)
        value = recv2[dt * high]
        for dh in range(1, high):
            value = value + recv2[dt * high + dh]
        out_ref[source] = value.astype(BF16)
    for d in range(1, groups):
        first_copy(d).wait_send()
    for d in range(1, ends):
        second_copy(d).wait_send()


def exchange(table_rows, keep, ids, lead, over, tables, groups, ends):
    rows, width = table_rows.shape[1:]
    batch = over.shape[0]
    part = batch // groups
    each = part // ends
    vmem = pl.BlockSpec(memory_space=pltpu.VMEM)
    return pl.pallas_call(
        functools.partial(exchange_kernel, tables),
        out_shape=jax.ShapeDtypeStruct((tables, each, width), BF16),
        in_specs=[pl.BlockSpec(memory_space=pltpu.HBM)] + [vmem] * 4,
        out_specs=vmem,
        scratch_shapes=[
            pltpu.VMEM((rows, width), BF16),
            pltpu.VMEM((rows, width), F32),
            pltpu.VMEM((KEEP * LANES, width), F32),
            pltpu.VMEM((batch, width), F32),
            pltpu.VMEM((groups, part, width), F32),
            pltpu.VMEM((ends, each, width), F32),
            pltpu.VMEM((ends, each, width), F32),
            pltpu.SMEM((KEEP + 8, LANES), I32),
            pltpu.SemaphoreType.DMA((4,)),
            pltpu.SemaphoreType.DMA,
            pltpu.SemaphoreType.DMA((groups,)),
            pltpu.SemaphoreType.DMA((groups,)),
            pltpu.SemaphoreType.DMA((ends,)),
            pltpu.SemaphoreType.DMA((ends,)),
        ],
        compiler_params=pltpu.CompilerParams(
            collective_id=0, has_side_effects=True, vmem_limit_bytes=24 * 1024 * 1024
        ),
        name="exchange",
    )(pltpu.with_memory_space_constraint(table_rows, pltpu.HBM), keep, ids, lead, over)


def on_device(tables, indices, weights, lengths):
    picked = rank(tables, indices, weights, lengths)
    return exchange(tables, *picked, lax.axis_size("table"), 32, 8)


def solution(mesh):
    placed = (
        P("table", "row", None),
        P("table", None, None),
        P("table", None, None),
        P("table", None),
    )
    return jax.shard_map(
        on_device,
        mesh=mesh,
        in_specs=placed,
        out_specs=P(None, ("table", "row"), None),
        check_vma=False,
    )
```
